256 devices in a mesh: field: 32 (over z, x), vrow: 2 (over core), vcol: 4 (over y).
Axes of the slice: x: 4, y: 4, z: 8, core: 2. Of those that a mesh axis runs over, the one named last changes fastest.
Arguments:
- blocks: bfloat16 [1024, 192, 2, 256], P(('vrow', 'vcol'), 'field'), may hold values from 0 to 1
- block_ids: int32 [8, 32, 6], P(('vrow', 'vcol'), 'field'), may hold values from 0 to 11, as said below
- block_counts: int32 [8, 32], P(('vrow', 'vcol'), 'field'), may hold values from 1 to 6, as said below
Outputs:
- tables: float32 [1024, 2, 2, 4, 2, 128], P(('vrow', 'field'), None, None, 'vcol')
The draws below stay inside these ranges and needn't reach their ends.
Inputs may be any that keep to these rules, and one draw needn't show every extreme that they name: `block_ids`: within each row of the last dimension the entries are distinct. `block_counts`: 6 is reached in every draw.
All inputs are finite; a program needn't handle non-finite values.
Results may differ from the reference program's by a relative error of at most 0.0003.
Values may be sent and summed in bfloat16 or wider, within the bound.
No kernel may reach another device: no remote copies, remote signals or barrier semaphores. Data moves between devices by JAX's collectives and lax.ppermute only.
A program may use at most 64 MiB of HBM per device.

```python
import jax
import jax.numpy as jnp
from jax import lax

VS = 128
SBLK = 12
BLOCK = 256
OCC = 6
NSH = 8
V = 1024
NSAMP = 98304
N_FIELD = 32
N_VROW = 2
N_VCOL = 4


def draw_block_ids(key, part):
    keys = jax.random.split(jax.random.fold_in(key, 11), NSH * N_FIELD)
    picks = jax.vmap(lambda k: jax.random.permutation(k, SBLK)[:OCC])(keys)
    return picks.reshape(NSH, N_FIELD, OCC).astype(jnp.int32)


def draw_block_counts(key, part):
    first = jax.random.fold_in(key, 23)
    values = jax.random.randint(first, (NSH * N_FIELD,), 1, OCC + 1)
    where = jax.random.randint(jax.random.fold_in(key, 29), (), 0, NSH * N_FIELD)
    values = values.at[where].set(OCC)
    return values.reshape(NSH, N_FIELD).astype(jnp.int32)


def block_levels(own_key, dims, shards, smallest, top_value):
    def one(axis_at, parts):
        heights = jax.random.uniform(jax.random.fold_in(jax.random.fold_in(own_key, 6), axis_at), (parts,), jnp.float32, smallest / len(shards), top_value / len(shards))
        return jnp.repeat(jnp.exp(heights), dims[axis_at] // parts).reshape((-1,) + (1,) * (len(dims) - axis_at - 1))

    gain = one(*shards[0])
    for cut in shards[1:]:
        gain = gain * one(*cut)
    return gain


def setup_inputs(seed: int = 0) -> dict:
    key_of = jax.random.split(jax.random.key(seed), 4)
    return {
        "blocks": jnp.clip(1.0 * jax.random.uniform(key_of[0], (V, N_FIELD * OCC, 2, BLOCK), jnp.float32) ** block_levels(key_of[0], (V, N_FIELD * OCC, 2, BLOCK), ((0, 8), (1, 32)), -0.2, 0.2), 0.0, 1.0).astype(jnp.bfloat16),
        "block_ids": draw_block_ids(jax.random.fold_in(key_of[3], 71), 0),
        "block_counts": draw_block_counts(jax.random.fold_in(key_of[3], 71), 0),
    }


def reference(blocks, block_ids, block_counts):
    occ = block_ids.shape[-1]
    shaped = blocks.reshape(NSH, VS, N_FIELD, occ, 2, BLOCK).astype(jnp.float32)
    slots = jnp.arange(occ, dtype=jnp.int32)
    live = slots[None, None, :] < block_counts[:, :, None]
    onehot = (block_ids[:, :, :, None] == jnp.arange(SBLK, dtype=jnp.int32)[None, None, None, :]) & live[..., None]
    dense = jnp.einsum('sfok,svfocx->svcfkx', onehot.astype(jnp.float32), shaped, precision=lax.Precision.HIGHEST)
    dense = dense.astype(jnp.bfloat16).reshape(NSH * VS * 2, N_FIELD * SBLK * BLOCK).astype(jnp.float32)
    prods = jnp.dot(dense, dense.T, precision=lax.Precision.HIGHEST)
    prods = prods / NSAMP
    prods = prods.reshape(NSH * VS, 2, N_VROW, N_VCOL, VS, 2)
    return jnp.transpose(prods, (0, 1, 2, 3, 5, 4))
```

```python
import functools

import jax
import jax.numpy as jnp
from jax import lax
from jax.experimental import pallas as pl
from jax.experimental.pallas import tpu as pltpu
from jax.sharding import Mesh, PartitionSpec as P

SBLK = 12
OCC = 6
BLOCK = 256
VS = 128
NX = 4
NSAMP = 98304


VM = pl.BlockSpec(memory_space=pltpu.VMEM)
SM = pl.BlockSpec(memory_space=pltpu.SMEM)


def rotate(array, axis, shift):
    n = lax.axis_size(axis)
    return lax.ppermute(array, axis, [(i, (i + shift) % n) for i in range(n)])


def table_kernel(n, halves, pos, own_ids, sib_ids, *refs):
    row_ids, refs = refs[:n], refs[n:]
    own, sib = refs[:2]
    rows, refs = refs[2 : 2 + n * halves], refs[2 + n * halves :]
    outs, (slot_of, acc) = refs[:NX], refs[NX:]
    x, core = pos[0], pos[1]
    for s, ids in enumerate((own_ids, sib_ids)):
        for k in range(SBLK + 1):
            slot_of[s, k] = -1
        for o in range(OCC):
            slot_of[s, ids[o]] = o
        slot_of[s, SBLK] = -1
    per = OCC // halves
    for j in range(n):
        for s, cols in enumerate((own, sib)):
            total = None
            for o in range(OCC):
                slot = slot_of[s, row_ids[j][o]]
                m = rows[j * halves + o // per][o % per]
                m = jnp.where(slot >= 0, m, jnp.zeros_like(m))
                c = cols[jnp.maximum(slot, 0)]
                d = lax.dot_general(
                    m, c, (((1,), (1,)), ((), ())), preferred_element_type=jnp.float32
                )
                total = d if total is None else total + d
            acc[s] = total
            r = core if s == 0 else 1 - core
            for k in range(NX):
                there = lax.rem(x + k, NX) * 16
                for zz in range(2):
                    for a in range(2):
                        at = pl.ds(pl.multiple_of(there + a * VS + zz * 64, 16), 16)
                        for b in range(2):
                            outs[k][j, r, b, pl.ds((zz * 2 + a) * 16, 16), :] = acc[
                                s, at, pl.ds(b * VS, VS)
                            ]


def tables(pos, own_ids, sib_ids, row_ids, own, sib, rows, halves=1):
    n = len(row_ids)
    piece = jax.ShapeDtypeStruct((n, 2, 2, 64, VS), jnp.float32)
    return pl.pallas_call(
        functools.partial(table_kernel, n, halves),
        out_shape=(piece,) * NX,
        in_specs=[SM] * (3 + n) + [VM] * (2 + len(rows)),
        out_specs=(VM,) * NX,
        scratch_shapes=[pltpu.SMEM((2, 16), jnp.int32), pltpu.VMEM((2, 256, 256), jnp.float32)],
    )(pos, own_ids, sib_ids, *row_ids, own, sib, *rows)


def sum_kernel(groups, pos, *refs):
    ins, out = refs[:-1], refs[-1]
    y = pos[2]
    g = 0
    for shifts in groups:
        for j, shift in enumerate(shifts):
            p = lax.rem(y + shift, 4)
            for zz in range(2):
                part = pl.ds(zz * 32, 32)
                total = ins[g * NX][j, :, :, part, :]
                for k in range(1, NX):
                    total = total + ins[g * NX + k][j, :, :, part, :]
                out[2 * p + zz] = total
        g += 1


def summed(pos, groups, pieces):
    return pl.pallas_call(
        functools.partial(sum_kernel, groups),
        out_shape=jax.ShapeDtypeStruct((8, 2, 2, 32, VS), jnp.float32),
        in_specs=[SM] + [VM] * len(pieces),
        out_specs=VM,
    )(pos, *pieces)


def last_kernel(parts, out):
    for r in range(2):
        for b in range(2):
            total = parts[0, r, b]
            for z in range(1, 8):
                total = total + parts[z, r, b]
            total = total / NSAMP
            for a in range(2):
                out[:, a, r, 0, b, :] = total[a * 16 : (a + 1) * 16]


def last(parts):
    return pl.pallas_call(
        last_kernel,
        out_shape=jax.ShapeDtypeStruct((16, 2, 2, 1, 2, VS), jnp.float32),
        in_specs=[VM],
        out_specs=VM,
    )(parts)


def on_device(blocks, block_ids, block_counts):
    pos = jnp.stack(
        [lax.axis_index("x"), lax.axis_index("vrow"), lax.axis_index("vcol"), 0]
    ).astype(jnp.int32)
    own = jnp.transpose(blocks, (1, 2, 0, 3)).reshape(OCC, 2 * VS, BLOCK)
    slots = jnp.arange(OCC, dtype=jnp.int32)
    ids = jnp.where(slots < block_counts[0, 0], block_ids[0, 0], SBLK)
    up = rotate(own, "vcol", -1)
    down = rotate(own, "vcol", 1)
    sib = rotate(own, "vrow", 1)
    sib_ids = rotate(ids, "vrow", 1)
    up_ids = rotate(ids, "vcol", -1)
    down_ids = rotate(ids, "vcol", 1)
    far_ids = rotate(ids, "vcol", 2)
    half = OCC // 2
    far_a = rotate(up[:half], "vcol", -1)
    far_b = rotate(down[half:], "vcol", 1)

    def exchanged(pieces):
        return [pieces[0]] + [rotate(pieces[k], "x", k) for k in range(1, NX)]

    here = exchanged(tables(pos, ids, sib_ids, [ids], own, sib, [own]))
    near = exchanged(tables(pos, ids, sib_ids, [up_ids, down_ids], own, sib, [up, down]))
    far = exchanged(tables(pos, ids, sib_ids, [far_ids], own, sib, [far_a, far_b], halves=2))
    parts = summed(pos, ((0,), (1, 3), (2,)), here + near + far)
    return last(lax.all_to_all(parts, "z", 0, 0, tiled=True))


def solution(mesh):
    fine = Mesh(mesh.devices.reshape(-1, NX, 2, 4), ("z", "x", "vrow", "vcol"))
    placed = (
        P(("vrow", "vcol"), ("z", "x"), None, None),
        P(("vrow", "vcol"), ("z", "x"), None),
        P(("vrow", "vcol"), ("z", "x")),
    )
    return jax.shard_map(
        on_device,
        mesh=fine,
        in_specs=placed,
        out_specs=P(("vrow", "z", "x"), None, None, "vcol", None, None),
        check_vma=False,
    )
```

```python
import functools

import jax
import jax.numpy as jnp
from jax import lax
from jax.experimental import pallas as pl
from jax.experimental.pallas import tpu as pltpu
from jax.sharding import Mesh, PartitionSpec as P


SBLK = 12
OCC = 6
HALF = OCC // 2
BLOCK = 256
VS = 128
ROWS = HALF * 2 * VS
PARTS = [pl.ds(v, 16) for v in range(0, VS, 16)]
NX = 4
NSAMP = 98304

STEPS = 2730.0
TOP = 32767.0
BIAS = 32768.0


VM = pl.BlockSpec(memory_space=pltpu.VMEM)


def on_chip(f, out_shape, arrays, scratch, flops, aliases={}):
    arrays = [pltpu.with_memory_space_constraint(a, pltpu.VMEM) for a in arrays]
    many = isinstance(out_shape, tuple)
    return pl.pallas_call(
        f,
        out_shape=out_shape,
        in_specs=[VM] * len(arrays),
        out_specs=(VM,) * len(out_shape) if many else VM,
        scratch_shapes=scratch,
        input_output_aliases=aliases,
        cost_estimate=pl.CostEstimate(flops=flops, transcendentals=0, bytes_accessed=0),
        compiler_params=pltpu.CompilerParams(vmem_limit_bytes=12 << 20),
    )(*arrays)


def rotate(array, axis, shift):
    n = lax.axis_size(axis)
    return lax.ppermute(array, axis, [(i, (i + shift) % n) for i in range(n)])


def exponent(largest):
    return jnp.clip(jnp.ceil(jnp.log2(largest)), -100.0, 100.0)


def coded(values, exp):
    q = jnp.round((exp - jnp.log2(values)) * STEPS) - BIAS
    q = jnp.clip(q, -BIAS, TOP)
    return q.astype(jnp.int32).astype(jnp.int16)


def decoded(codes, exp):
    q = codes.astype(jnp.int32).astype(jnp.float32)
    return jnp.where(q >= TOP, 0.0, jnp.exp2((exp - BIAS / STEPS) - q * (1.0 / STEPS)))


def relay_kernel(blocks, a, b, held, sems):
    copies = [
        pltpu.make_async_copy(blocks.at[part], held.at[part], sems.at[i])
        for i, part in enumerate(PARTS)
    ]
    for copy in copies:
        copy.start()
    for part, copy in zip(PARTS, copies):
        copy.wait()
        for o in range(OCC):
            both = jnp.swapaxes(held[part, o], 0, 1)
            for c in range(2):
                to = (o % HALF) * 2 * VS + c * VS + part.start
                (a, b)[o // HALF][to : to + part.size, :] = both[c]


def relaid(blocks):
    half = pltpu.VMEM((ROWS, BLOCK), jnp.bfloat16)
    return pl.pallas_call(
        relay_kernel,
        out_shape=(half,) * 2,
        in_specs=[pl.BlockSpec(memory_space=pltpu.HBM)],
        out_specs=(VM,) * 2,
        scratch_shapes=[
            pltpu.VMEM(blocks.shape, jnp.bfloat16),
            pltpu.SemaphoreType.DMA((len(PARTS),)),
        ],
        compiler_params=pltpu.CompilerParams(vmem_limit_bytes=12 << 20),
    )(pltpu.with_memory_space_constraint(blocks, pltpu.HBM))


def tag_kernel(ids, count, a, b, tagged_a, tagged_b, tags):
    lane = lax.broadcasted_iota(jnp.int32, (16, BLOCK), 1)
    word = jnp.full((16, BLOCK), SBLK, jnp.int32)
    for o in range(OCC):
        word = jnp.where((lane == o) & (o < count[0]), ids[o], word)
    word = word.astype(jnp.float32).astype(jnp.bfloat16)
    tags[...] = word
    for half, out in ((a, tagged_a), (b, tagged_b)):
        out[:ROWS] = half[...]
        out[ROWS:] = word


def tagged(ids, count, halves):
    more = pltpu.VMEM((ROWS + 16, BLOCK), jnp.bfloat16)
    smem = pl.BlockSpec(memory_space=pltpu.SMEM)
    return pl.pallas_call(
        tag_kernel,
        out_shape=(more, more, pltpu.VMEM((16, BLOCK), jnp.bfloat16)),
        in_specs=[smem, smem, VM, VM],
        out_specs=(VM,) * 3,
        cost_estimate=pl.CostEstimate(flops=2 * 256**3, transcendentals=0, bytes_accessed=0),
        compiler_params=pltpu.CompilerParams(vmem_limit_bytes=12 << 20),
    )(ids, count, *(pltpu.with_memory_space_constraint(h, pltpu.VMEM) for h in halves))


def ids_of(ref):
    at = ref.shape[0] - 16
    tags = ref[at : at + 16, :VS].astype(jnp.float32)[:1]
    lane = lax.broadcasted_iota(jnp.int32, (1, VS), 1)
    weight = jnp.zeros((1, VS), jnp.float32)
    for o in range(OCC):
        weight = jnp.where(lane == o, float(16**o), weight)
    word = jnp.sum(tags * weight).astype(jnp.int32)
    return [(word >> (4 * o)) & 15 for o in range(OCC)]


def table_kernel(n, gathers, *refs):
    col_tags, row_tags, refs = refs[:2], refs[2 : 2 + n], refs[2 + n :]
    if gathers:
        (a0, b0, a1, b1), refs = refs[:4], refs[4:]
        rows = (a0, b0)
    else:
        cols, rows, refs = refs[0], refs[1 : 1 + 2 * n], refs[1 + 2 * n :]
    outs, refs = refs[:NX], refs[NX:]
    if gathers:
        cols, refs = refs[0], refs[1:]
        for s, halves in enumerate(((a0, b0), (a1, b1))):
            for o in range(OCC):
                cols[s, o] = halves[o // HALF][pl.ds((o % HALF) * 256, 256), :]
    slot_of, acc = refs
    x, core = lax.axis_index("x"), lax.axis_index("vrow")
    for s, ref in enumerate(col_tags):
        ids = ids_of(ref)
        for k in range(SBLK + 1):
            slot_of[s, k] = -1
        for o in range(OCC):
            slot_of[s, ids[o]] = o
        slot_of[s, SBLK] = -1
    row_ids = [ids_of(ref) for ref in row_tags]
    for j in range(n):
        largest = None
        for s in range(2):
            total = None
            for o in range(OCC):
                slot = slot_of[s, row_ids[j][o]]
                m = rows[2 * j + o // HALF][pl.ds((o % HALF) * 256, 256), :]
                m = jnp.where(slot >= 0, m, jnp.zeros_like(m))
                d = lax.dot_general(
                    m,
                    cols[s, jnp.maximum(slot, 0)],
                    (((1,), (1,)), ((), ())),
                    preferred_element_type=jnp.float32,
                )
                total = d if total is None else total + d
            acc[s] = total
            top = jnp.max(total)
            largest = top if largest is None else jnp.maximum(largest, top)
        exp = exponent(jnp.full((16, VS), largest, jnp.float32))
        for k in range(1, NX):
            outs[k][j, 256:272, :] = exp.astype(jnp.int32).astype(jnp.int16)
        for s in range(2):
            r = core if s == 0 else 1 - core
            for k in range(NX):
                there = lax.rem(x + k, NX) * 16
                for zz in range(2):
                    for a in range(2):
                        at = pl.ds(pl.multiple_of(there + a * VS + zz * 64, 16), 16)
                        for b in range(2):
                            v = acc[s, at, pl.ds(b * VS, VS)]
                            to = pl.multiple_of(r * 128 + (b * 64 + (zz * 2 + a) * 16), 16)
                            if k:
                                v = coded(v, exp)
                            outs[k][j, pl.ds(to, 16), :] = v


def tables(col_tags, row_tags, arrays, gathers=False):
    n = len(row_tags)
    kept = pltpu.VMEM((n, 256, VS), jnp.float32)
    sent = pltpu.VMEM((n, 272, VS), jnp.int16)
    outs = (kept,) + (sent,) * (NX - 1)
    if gathers:
        outs += (pltpu.VMEM((2, OCC, 2 * VS, BLOCK), jnp.bfloat16),)
    return on_chip(
        functools.partial(table_kernel, n, gathers),
        outs,
        [*col_tags, *row_tags, *arrays],
        [pltpu.SMEM((2, 16), jnp.int32), pltpu.VMEM((2, 256, 256), jnp.float32)],
        n * 12 * 2 * 256**3,
    )


def sum_kernel(n, shifts, *refs):
    ins, (out, acc) = refs[: n * NX], refs[-2:]
    y = lax.axis_index("vcol")
    for g, group in enumerate(shifts):
        mine = ins[g * NX : g * NX + NX]
        for j, shift in enumerate(group):
            p = lax.rem(y + shift, 4)
            exps = [mine[k][j, 256:272, :].astype(jnp.int32).astype(jnp.float32)[:1] for k in range(1, NX)]
            largest = None
            for rb in range(4):
                part = pl.ds(rb * 64, 64)
                total = mine[0][j, part, :]
                for k in range(1, NX):
                    total = total + decoded(mine[k][j, part, :], exps[k - 1])
                acc[part, :] = total
                largest = total if largest is None else jnp.maximum(largest, total)
            exp = exponent(jnp.full((16, VS), jnp.max(largest), jnp.float32))
            for zz in range(2):
                to = 2 * p + zz
                out[to, 128:144, :] = exp.astype(jnp.int32).astype(jnp.int16)
                for rb in range(4):
                    v = acc[pl.ds(rb * 64 + zz * 32, 32), :]
                    out[to, rb * 32 : rb * 32 + 32, :] = coded(v, exp[:1])


def summed(shifts, pieces, base=None):
    n = len(shifts)
    extra = [] if base is None else [base]
    return on_chip(
        functools.partial(sum_kernel, n, shifts),
        pltpu.VMEM((8, 144, VS), jnp.int16),
        pieces + extra,
        [pltpu.VMEM((256, VS), jnp.float32)],
        12 * 2 * 256**3,
        {} if base is None else {len(pieces): 0},
    )


def last_kernel(parts, out):
    exps = [
        parts[z, 128:144, :].astype(jnp.int32).astype(jnp.float32)[:1] for z in range(8)
    ]
    for r in range(2):
        for b in range(2):
            part = pl.ds((r * 2 + b) * 32, 32)
            total = decoded(parts[0, part, :], exps[0])
            for z in range(1, 8):
                total = total + decoded(parts[z, part, :], exps[z])
            total = total / NSAMP
            for a in range(2):
                out[:, a, r, 0, b, :] = total[a * 16 : (a + 1) * 16]


def last(parts):
    return on_chip(
        last_kernel,
        jax.ShapeDtypeStruct((16, 2, 2, 1, 2, VS), jnp.float32),
        [parts],
        [],
        2 * 256**3,
    )


def on_device(blocks, block_ids, block_counts):
    a, b = relaid(blocks)
    tagged_a, tagged_b, tags = tagged(block_ids.reshape(OCC), block_counts.reshape(1), (a, b))
    up = [rotate(a, "vcol", -1), rotate(tagged_b, "vcol", -1)]
    down = [rotate(tagged_a, "vcol", 1), rotate(b, "vcol", 1)]
    sib = [rotate(a, "vrow", 1), rotate(tagged_b, "vrow", 1)]
    far_tags = rotate(tags, "vcol", 2)
    second = [rotate(up[0], "vcol", -1), rotate(down[1], "vcol", 1)]
    col_tags = [tags, sib[1]]

    def exchanged(pieces):
        return [pieces[0]] + [rotate(pieces[k], "x", k) for k in (1, 2, 3)]

    *here, cols = tables(col_tags, [tags], [a, b, *sib], gathers=True)
    near = tables(col_tags, [up[1], down[0]], [cols, *up, *down])
    far = tables(col_tags, [far_tags], [cols, *second])
    here, near, far = (
        exchanged(pieces) for pieces in (here, near, far)
    )
    parts = summed(((0,), (1, 3)), here + near)
    parts = summed(((2,),), far, parts)
    parts = lax.all_to_all(parts, "z", 0, 0, tiled=True)
    return last(parts)


def solution(mesh):
    fine = Mesh(mesh.devices.reshape(-1, NX, 2, 4), ("z", "x", "vrow", "vcol"))
    field = ("z", "x")
    held = (
        P(("vrow", "vcol"), field, None, None),
        P(("vrow", "vcol"), field, None),
        P(("vrow", "vcol"), field),
    )
    return jax.shard_map(
        on_device,
        mesh=fine,
        in_specs=held,
        out_specs=P(("vrow", *field), None, None, "vcol", None, None),
        check_vma=False,
    )
```

```python
import functools

import jax
import jax.numpy as jnp
from jax import lax
from jax.experimental import pallas as pl
from jax.experimental.pallas import tpu as pltpu
from jax.sharding import Mesh, PartitionSpec as P


SBLK = 12
OCC = 6
HALF = OCC // 2
BLOCK = 256
VS = 128
ROWS = HALF * 2 * VS
PARTS = [pl.ds(v, 16) for v in range(0, VS, 16)]
NX = 4
NSAMP = 98304

STEPS = 2730.0
TOP = 32767.0
BIAS = 32768.0


VM = pl.BlockSpec(memory_space=pltpu.VMEM)


def on_chip(f, out_shape, arrays, scratch, flops, aliases={}):
    arrays = [pltpu.with_memory_space_constraint(a, pltpu.VMEM) for a in arrays]
    many = isinstance(out_shape, tuple)
    return pl.pallas_call(
        f,
        out_shape=out_shape,
        in_specs=[VM] * len(arrays),
        out_specs=(VM,) * len(out_shape) if many else VM,
        scratch_shapes=scratch,
        input_output_aliases=aliases,
        cost_estimate=pl.CostEstimate(flops=flops, transcendentals=0, bytes_accessed=0),
        compiler_params=pltpu.CompilerParams(vmem_limit_bytes=12 << 20),
    )(*arrays)


def rotate(array, axis, shift):
    n = lax.axis_size(axis)
    return lax.ppermute(array, axis, [(i, i ^ shift) for i in range(n)])


def exponent(largest):
    return jnp.clip(jnp.ceil(jnp.log2(largest)), -100.0, 100.0)


def coded(values, exp):
    q = jnp.round((exp - jnp.log2(values)) * STEPS) - BIAS
    q = jnp.clip(q, -BIAS, TOP)
    return q.astype(jnp.int32).astype(jnp.int16)


def decoded(codes, exp):
    q = codes.astype(jnp.int32).astype(jnp.float32)
    return jnp.where(q >= TOP, 0.0, jnp.exp2((exp - BIAS / STEPS) - q * (1.0 / STEPS)))


def relay_kernel(blocks, a, b, held, sems):
    copies = [
        pltpu.make_async_copy(blocks.at[part], held.at[part], sems.at[i])
        for i, part in enumerate(PARTS)
    ]
    for copy in copies:
        copy.start()
    for part, copy in zip(PARTS, copies):
        copy.wait()
        for o in range(OCC):
            both = jnp.swapaxes(held[part, o], 0, 1)
            for c in range(2):
                to = (o % HALF) * 2 * VS + c * VS + part.start
                (a, b)[o // HALF][to : to + part.size, :] = both[c]


def relaid(blocks):
    half = pltpu.VMEM((ROWS, BLOCK), jnp.bfloat16)
    return pl.pallas_call(
        relay_kernel,
        out_shape=(half,) * 2,
        in_specs=[pl.BlockSpec(memory_space=pltpu.HBM)],
        out_specs=(VM,) * 2,
        scratch_shapes=[
            pltpu.VMEM(blocks.shape, jnp.bfloat16),
            pltpu.SemaphoreType.DMA((len(PARTS),)),
        ],
        compiler_params=pltpu.CompilerParams(vmem_limit_bytes=12 << 20),
    )(pltpu.with_memory_space_constraint(blocks, pltpu.HBM))


def tag_kernel(ids, count, a, b, tagged_a, tagged_b, tags):
    lane = lax.broadcasted_iota(jnp.int32, (16, BLOCK), 1)
    word = jnp.full((16, BLOCK), SBLK, jnp.int32)
    for o in range(OCC):
        word = jnp.where((lane == o) & (o < count[0]), ids[o], word)
    word = word.astype(jnp.float32).astype(jnp.bfloat16)
    tags[...] = word
    for half, out in ((a, tagged_a), (b, tagged_b)):
        out[:ROWS] = half[...]
        out[ROWS:] = word


def tagged(ids, count, halves):
    more = pltpu.VMEM((ROWS + 16, BLOCK), jnp.bfloat16)
    smem = pl.BlockSpec(memory_space=pltpu.SMEM)
    return pl.pallas_call(
        tag_kernel,
        out_shape=(more, more, pltpu.VMEM((16, BLOCK), jnp.bfloat16)),
        in_specs=[smem, smem, VM, VM],
        out_specs=(VM,) * 3,
        cost_estimate=pl.CostEstimate(flops=2 * 256**3, transcendentals=0, bytes_accessed=0),
        compiler_params=pltpu.CompilerParams(vmem_limit_bytes=12 << 20),
    )(ids, count, *(pltpu.with_memory_space_constraint(h, pltpu.VMEM) for h in halves))


def ids_of(ref):
    at = ref.shape[0] - 16
    tags = ref[at : at + 16, :VS].astype(jnp.float32)[:1]
    lane = lax.broadcasted_iota(jnp.int32, (1, VS), 1)
    weight = jnp.zeros((1, VS), jnp.float32)
    for o in range(OCC):
        weight = jnp.where(lane == o, float(16**o), weight)
    word = jnp.sum(tags * weight).astype(jnp.int32)
    return [(word >> (4 * o)) & 15 for o in range(OCC)]


def table_kernel(n, gathers, *refs):
    col_tags, row_tags, refs = refs[:2], refs[2 : 2 + n], refs[2 + n :]
    if gathers:
        (a0, b0, a1, b1), refs = refs[:4], refs[4:]
        rows = (a0, b0)
    else:
        cols, rows, refs = refs[0], refs[1 : 1 + 2 * n], refs[1 + 2 * n :]
    outs, refs = refs[:NX], refs[NX:]
    if gathers:
        cols, refs = refs[0], refs[1:]
        for s, halves in enumerate(((a0, b0), (a1, b1))):
            for o in range(OCC):
                cols[s, o] = halves[o // HALF][pl.ds((o % HALF) * 256, 256), :]
    slot_of, acc = refs
    x, core = lax.axis_index("x"), lax.axis_index("vrow")
    for s, ref in enumerate(col_tags):
        ids = ids_of(ref)
        for k in range(SBLK + 1):
            slot_of[s, k] = -1
        for o in range(OCC):
            slot_of[s, ids[o]] = o
        slot_of[s, SBLK] = -1
    row_ids = [ids_of(ref) for ref in row_tags]
    for j in range(n):
        largest = None
        for s in range(2):
            total = None
            for o in range(OCC):
                slot = slot_of[s, row_ids[j][o]]
                m = rows[2 * j + o // HALF][pl.ds((o % HALF) * 256, 256), :]
                m = jnp.where(slot >= 0, m, jnp.zeros_like(m))
                d = lax.dot_general(
                    m,
                    cols[s, jnp.maximum(slot, 0)],
                    (((1,), (1,)), ((), ())),
                    preferred_element_type=jnp.float32,
                )
                total = d if total is None else total + d
            acc[s] = total
            top = jnp.max(total)
            largest = top if largest is None else jnp.maximum(largest, top)
        exp = exponent(jnp.full((16, VS), largest, jnp.float32))
        for k in range(1, NX):
            outs[k][j, 256:272, :] = exp.astype(jnp.int32).astype(jnp.int16)
        for s in range(2):
            r = core if s == 0 else 1 - core
            for k in range(NX):
                there = lax.bitwise_xor(x, k) * 16
                for zz in range(2):
                    for a in range(2):
                        at = pl.ds(pl.multiple_of(there + a * VS + zz * 64, 16), 16)
                        for b in range(2):
                            v = acc[s, at, pl.ds(b * VS, VS)]
                            to = pl.multiple_of(r * 128 + (b * 64 + (zz * 2 + a) * 16), 16)
                            if k:
                                v = coded(v, exp)
                            outs[k][j, pl.ds(to, 16), :] = v


def tables(col_tags, row_tags, arrays, gathers=False):
    n = len(row_tags)
    kept = pltpu.VMEM((n, 256, VS), jnp.float32)
    sent = pltpu.VMEM((n, 272, VS), jnp.int16)
    outs = (kept,) + (sent,) * (NX - 1)
    if gathers:
        outs += (pltpu.VMEM((2, OCC, 2 * VS, BLOCK), jnp.bfloat16),)
    return on_chip(
        functools.partial(table_kernel, n, gathers),
        outs,
        [*col_tags, *row_tags, *arrays],
        [pltpu.SMEM((2, 16), jnp.int32), pltpu.VMEM((2, 256, 256), jnp.float32)],
        n * 12 * 2 * 256**3,
    )


def sum_kernel(n, shifts, *refs):
    ins, (out, acc) = refs[: n * NX], refs[-2:]
    y = lax.axis_index("vcol")
    for g, group in enumerate(shifts):
        mine = ins[g * NX : g * NX + NX]
        for j, shift in enumerate(group):
            p = lax.bitwise_xor(y, shift)
            exps = [mine[k][j, 256:272, :].astype(jnp.int32).astype(jnp.float32)[:1] for k in range(1, NX)]
            largest = None
            for rb in range(4):
                part = pl.ds(rb * 64, 64)
                total = mine[0][j, part, :]
                for k in range(1, NX):
                    total = total + decoded(mine[k][j, part, :], exps[k - 1])
                acc[part, :] = total
                largest = total if largest is None else jnp.maximum(largest, total)
            exp = exponent(jnp.full((16, VS), jnp.max(largest), jnp.float32))
            for zz in range(2):
                to = 2 * p + zz
                out[to, 128:144, :] = exp.astype(jnp.int32).astype(jnp.int16)
                for rb in range(4):
                    v = acc[pl.ds(rb * 64 + zz * 32, 32), :]
                    out[to, rb * 32 : rb * 32 + 32, :] = coded(v, exp[:1])


def summed(shifts, pieces, base=None):
    n = len(shifts)
    extra = [] if base is None else [base]
    return on_chip(
        functools.partial(sum_kernel, n, shifts),
        pltpu.VMEM((8, 144, VS), jnp.int16),
        pieces + extra,
        [pltpu.VMEM((256, VS), jnp.float32)],
        12 * 2 * 256**3,
        {} if base is None else {len(pieces): 0},
    )


def last_kernel(parts, out):
    exps = [
        parts[z, 128:144, :].astype(jnp.int32).astype(jnp.float32)[:1] for z in range(8)
    ]
    for r in range(2):
        for b in range(2):
            part = pl.ds((r * 2 + b) * 32, 32)
            total = decoded(parts[0, part, :], exps[0])
            for z in range(1, 8):
                total = total + decoded(parts[z, part, :], exps[z])
            total = total / NSAMP
            for a in range(2):
                out[:, a, r, 0, b, :] = total[a * 16 : (a + 1) * 16]


def last(parts):
    return on_chip(
        last_kernel,
        jax.ShapeDtypeStruct((16, 2, 2, 1, 2, VS), jnp.float32),
        [parts],
        [],
        2 * 256**3,
    )


def on_device(blocks, block_ids, block_counts):
    a, b = relaid(blocks)
    tagged_a, tagged_b, tags = tagged(block_ids.reshape(OCC), block_counts.reshape(1), (a, b))
    up = [rotate(a, "vcol", 1), rotate(tagged_b, "vcol", 1)]
    down = [rotate(tagged_a, "vcol", 3), rotate(b, "vcol", 3)]
    sib = [rotate(a, "vrow", 1), rotate(tagged_b, "vrow", 1)]
    far_tags = rotate(tags, "vcol", 2)
    second = [rotate(up[0], "vcol", 3), rotate(down[1], "vcol", 1)]
    col_tags = [tags, sib[1]]

    def exchanged(pieces):
        return [pieces[0]] + [rotate(pieces[k], "x", k) for k in (1, 2, 3)]

    *here, cols = tables(col_tags, [tags], [a, b, *sib], gathers=True)
    near = tables(col_tags, [up[1], down[0]], [cols, *up, *down])
    far = tables(col_tags, [far_tags], [cols, *second])
    here, near, far = (
        exchanged(pieces) for pieces in (here, near, far)
    )
    parts = summed(((0,), (1, 3)), here + near)
    parts = summed(((2,),), far, parts)
    parts = lax.all_to_all(parts, "z", 0, 0, tiled=True)
    return last(parts)


def solution(mesh):
    fine = Mesh(mesh.devices.reshape(-1, NX, 2, 4), ("z", "x", "vrow", "vcol"))
    field = ("z", "x")
    held = (
        P(("vrow", "vcol"), field, None, None),
        P(("vrow", "vcol"), field, None),
        P(("vrow", "vcol"), field),
    )
    return jax.shard_map(
        on_device,
        mesh=fine,
        in_specs=held,
        out_specs=P(("vrow", *field), None, None, "vcol", None, None),
        check_vma=False,
    )
```

```python
import functools

import jax
import jax.numpy as jnp
from jax import lax
from jax.experimental import pallas as pl
from jax.experimental.pallas import tpu as pltpu
from jax.sharding import Mesh, PartitionSpec as P


SBLK = 12
OCC = 6
HALF = OCC // 2
BLOCK = 256
VS = 128
ROWS = HALF * 2 * VS
PARTS = [pl.ds(v, 16) for v in range(0, VS, 16)]
NX = 4
NSAMP = 98304

STEPS = 2730.0
TOP = 32767.0
BIAS = 32768.0


VM = pl.BlockSpec(memory_space=pltpu.VMEM)


def on_chip(f, out_shape, arrays, scratch, flops, aliases={}):
    arrays = [pltpu.with_memory_space_constraint(a, pltpu.VMEM) for a in arrays]
    many = isinstance(out_shape, tuple)
    return pl.pallas_call(
        f,
        out_shape=out_shape,
        in_specs=[VM] * len(arrays),
        out_specs=(VM,) * len(out_shape) if many else VM,
        scratch_shapes=scratch,
        input_output_aliases=aliases,
        cost_estimate=pl.CostEstimate(flops=flops, transcendentals=0, bytes_accessed=0),
        compiler_params=pltpu.CompilerParams(vmem_limit_bytes=12 << 20),
    )(*arrays)


def rotate(array, axis, shift):
    n = lax.axis_size(axis)
    return lax.ppermute(array, axis, [(i, i ^ shift) for i in range(n)])


def exponent(largest):
    return jnp.clip(jnp.ceil(jnp.log2(largest)), -100.0, 100.0)


def coded(values, exp):
    q = jnp.round((exp - jnp.log2(values)) * STEPS) - BIAS
    q = jnp.clip(q, -BIAS, TOP)
    return q.astype(jnp.int32).astype(jnp.int16)


def decoded(codes, exp):
    q = codes.astype(jnp.int32).astype(jnp.float32)
    return jnp.where(q >= TOP, 0.0, jnp.exp2((exp - BIAS / STEPS) - q * (1.0 / STEPS)))


def relay_kernel(blocks, a, b, held, sems):
    copies = [
        pltpu.make_async_copy(blocks.at[part], held.at[part], sems.at[i])
        for i, part in enumerate(PARTS)
    ]
    for copy in copies:
        copy.start()
    for part, copy in zip(PARTS, copies):
        copy.wait()
        for o in range(OCC):
            both = jnp.swapaxes(held[part, o], 0, 1)
            for c in range(2):
                to = (o % HALF) * 2 * VS + c * VS + part.start
                (a, b)[o // HALF][to : to + part.size, :] = both[c]


def relaid(blocks):
    half = pltpu.VMEM((ROWS, BLOCK), jnp.bfloat16)
    return pl.pallas_call(
        relay_kernel,
        out_shape=(half,) * 2,
        in_specs=[pl.BlockSpec(memory_space=pltpu.HBM)],
        out_specs=(VM,) * 2,
        scratch_shapes=[
            pltpu.VMEM(blocks.shape, jnp.bfloat16),
            pltpu.SemaphoreType.DMA((len(PARTS),)),
        ],
        compiler_params=pltpu.CompilerParams(vmem_limit_bytes=12 << 20),
    )(pltpu.with_memory_space_constraint(blocks, pltpu.HBM))


def tag_kernel(ids, count, a, b, tagged_a, tagged_b, tags):
    lane = lax.broadcasted_iota(jnp.int32, (16, BLOCK), 1)
    word = jnp.full((16, BLOCK), SBLK, jnp.int32)
    for o in range(OCC):
        word = jnp.where((lane == o) & (o < count[0]), ids[o], word)
    word = word.astype(jnp.float32).astype(jnp.bfloat16)
    tags[...] = word
    for half, out in ((a, tagged_a), (b, tagged_b)):
        out[:ROWS] = half[...]
        out[ROWS:] = word


def tagged(ids, count, halves):
    more = pltpu.VMEM((ROWS + 16, BLOCK), jnp.bfloat16)
    smem = pl.BlockSpec(memory_space=pltpu.SMEM)
    return pl.pallas_call(
        tag_kernel,
        out_shape=(more, more, pltpu.VMEM((16, BLOCK), jnp.bfloat16)),
        in_specs=[smem, smem, VM, VM],
        out_specs=(VM,) * 3,
        cost_estimate=pl.CostEstimate(flops=2 * 256**3, transcendentals=0, bytes_accessed=0),
        compiler_params=pltpu.CompilerParams(vmem_limit_bytes=12 << 20),
    )(ids, count, *(pltpu.with_memory_space_constraint(h, pltpu.VMEM) for h in halves))


def ids_of(ref):
    at = ref.shape[0] - 16
    tags = ref[at : at + 16, :VS].astype(jnp.float32)[:1]
    lane = lax.broadcasted_iota(jnp.int32, (1, VS), 1)
    weight = jnp.zeros((1, VS), jnp.float32)
    for o in range(OCC):
        weight = jnp.where(lane == o, float(16**o), weight)
    word = jnp.sum(tags * weight).astype(jnp.int32)
    return [(word >> (4 * o)) & 15 for o in range(OCC)]


def table_kernel(n, gathers, *refs):
    col_tags, row_tags, refs = refs[:2], refs[2 : 2 + n], refs[2 + n :]
    if gathers:
        (a0, b0, a1, b1), refs = refs[:4], refs[4:]
        rows = (a0, b0)
    else:
        cols, rows, refs = refs[0], refs[1 : 1 + 2 * n], refs[1 + 2 * n :]
    outs, refs = refs[:NX], refs[NX:]
    if gathers:
        cols, refs = refs[0], refs[1:]
        for s, halves in enumerate(((a0, b0), (a1, b1))):
            for o in range(OCC):
                cols[s, o] = halves[o // HALF][pl.ds((o % HALF) * 256, 256), :]
    slot_of, acc = refs
    x, core = lax.axis_index("x"), lax.axis_index("vrow")
    for s, ref in enumerate(col_tags):
        ids = ids_of(ref)
        for k in range(SBLK + 1):
            slot_of[s, k] = -1
        for o in range(OCC):
            slot_of[s, ids[o]] = o
        slot_of[s, SBLK] = -1
    row_ids = [ids_of(ref) for ref in row_tags]
    for j in range(n):
        largest = None
        for s in range(2):
            total = None
            for o in range(OCC):
                slot = slot_of[s, row_ids[j][o]]
                m = rows[2 * j + o // HALF][pl.ds((o % HALF) * 256, 256), :]
                m = jnp.where(slot >= 0, m, jnp.zeros_like(m))
                d = lax.dot_general(
                    m,
                    cols[s, jnp.maximum(slot, 0)],
                    (((1,), (1,)), ((), ())),
                    preferred_element_type=jnp.float32,
                )
                total = d if total is None else total + d
            acc[s] = total
            top = jnp.max(total)
            largest = top if largest is None else jnp.maximum(largest, top)
        exp = exponent(jnp.full((16, VS), largest, jnp.float32))
        for k in range(1, NX):
            outs[k][j, 256:272, :] = exp.astype(jnp.int32).astype(jnp.int16)
        for s in range(2):
            r = core if s == 0 else 1 - core
            for k in range(NX):
                there = lax.bitwise_xor(x, k) * 16
                for zz in range(2):
                    for a in range(2):
                        at = pl.ds(pl.multiple_of(there + a * VS + zz * 64, 16), 16)
                        for b in range(2):
                            v = acc[s, at, pl.ds(b * VS, VS)]
                            to = pl.multiple_of(r * 128 + (b * 64 + (zz * 2 + a) * 16), 16)
                            if k:
                                v = coded(v, exp)
                            outs[k][j, pl.ds(to, 16), :] = v


def tables(col_tags, row_tags, arrays, gathers=False):
    n = len(row_tags)
    kept = pltpu.VMEM((n, 256, VS), jnp.float32)
    sent = pltpu.VMEM((n, 272, VS), jnp.int16)
    outs = (kept,) + (sent,) * (NX - 1)
    if gathers:
        outs += (pltpu.VMEM((2, OCC, 2 * VS, BLOCK), jnp.bfloat16),)
    return on_chip(
        functools.partial(table_kernel, n, gathers),
        outs,
        [*col_tags, *row_tags, *arrays],
        [pltpu.SMEM((2, 16), jnp.int32), pltpu.VMEM((2, 256, 256), jnp.float32)],
        n * 12 * 2 * 256**3,
    )


def sum_kernel(n, *refs):
    mine, (kept, sent) = refs[:NX], refs[NX:]
    zz = lax.axis_index("zz")
    for j in range(n):
        exps = [
            mine[k][j, 256:272, :].astype(jnp.int32).astype(jnp.float32)[:1] for k in range(1, NX)
        ]
        for half, out in ((zz, kept), (1 - zz, sent)):
            for rb in range(4):
                part = pl.ds(pl.multiple_of(rb * 64 + half * 32, 32), 32)
                total = mine[0][j, part, :]
                for k in range(1, NX):
                    total = total + decoded(mine[k][j, part, :], exps[k - 1])
                out[j, rb * 32 : rb * 32 + 32, :] = total


def summed(pieces):
    n = pieces[0].shape[0]
    return on_chip(
        functools.partial(sum_kernel, n),
        (pltpu.VMEM((n, 128, VS), jnp.float32),) * 2,
        pieces,
        [],
        n * 4 * 2 * 256**3,
    )


def pair_kernel(shifts, *refs):
    g = len(shifts)
    ins, outs, (acc, exps) = refs[: 2 * g], refs[2 * g : 2 * g + 4], refs[2 * g + 4 :]
    y, zh = lax.axis_index("vcol"), lax.axis_index("zh")
    for i, group in enumerate(shifts):
        for j, shift in enumerate(group):
            p = lax.bitwise_xor(y, shift)
            total = ins[2 * i][j] + ins[2 * i + 1][j]
            acc[p] = total
            exps[p] = exponent(jnp.full((16, VS), jnp.max(total), jnp.float32))
    outs[0][...] = acc[zh]
    for m in range(1, 4):
        p = lax.bitwise_xor(zh, m)
        exp = exps[p]
        outs[m][128:144, :] = exp.astype(jnp.int32).astype(jnp.int16)
        for part in range(4):
            rows = pl.ds(part * 32, 32)
            outs[m][rows, :] = coded(acc[p, rows, :], exp[:1])


def paired(shifts, pieces):
    return on_chip(
        functools.partial(pair_kernel, shifts),
        (pltpu.VMEM((128, VS), jnp.float32),) + (pltpu.VMEM((144, VS), jnp.int16),) * 3,
        pieces,
        [pltpu.VMEM((4, 128, VS), jnp.float32), pltpu.VMEM((4, 16, VS), jnp.float32)],
        6 * 2 * 256**3,
    )


def last_kernel(*refs):
    parts, out = refs[:4], refs[4]
    exps = [parts[m][128:144, :].astype(jnp.int32).astype(jnp.float32)[:1] for m in range(1, 4)]
    for r in range(2):
        for b in range(2):
            rows = pl.ds((r * 2 + b) * 32, 32)
            total = parts[0][rows, :]
            for m in range(1, 4):
                total = total + decoded(parts[m][rows, :], exps[m - 1])
            total = total / NSAMP
            for a in range(2):
                out[:, a, r, 0, b, :] = total[a * 16 : (a + 1) * 16]


def last(parts):
    return on_chip(
        last_kernel,
        jax.ShapeDtypeStruct((16, 2, 2, 1, 2, VS), jnp.float32),
        parts,
        [],
        2 * 256**3,
    )


def on_device(blocks, block_ids, block_counts):
    a, b = relaid(blocks)
    tagged_a, tagged_b, tags = tagged(block_ids.reshape(OCC), block_counts.reshape(1), (a, b))
    up = [rotate(a, "vcol", 1), rotate(tagged_b, "vcol", 1)]
    down = [rotate(tagged_a, "vcol", 3), rotate(b, "vcol", 3)]
    sib = [rotate(a, "vrow", 1), rotate(tagged_b, "vrow", 1)]
    far_tags = rotate(tags, "vcol", 2)
    second = [rotate(up[0], "vcol", 3), rotate(down[1], "vcol", 1)]
    col_tags = [tags, sib[1]]

    def exchanged(pieces):
        return [pieces[0]] + [rotate(pieces[k], "x", k) for k in (1, 2, 3)]

    *here, cols = tables(col_tags, [tags], [a, b, *sib], gathers=True)
    near = tables(col_tags, [up[1], down[0]], [cols, *up, *down])
    far = tables(col_tags, [far_tags], [cols, *second])
    parts = []
    for pieces in (here, near, far):
        pieces = exchanged(pieces)
        kept, sent = summed(pieces)
        parts += [kept, rotate(sent, "zz", 1)]
    kept, *sent = paired(((0,), (1, 3), (2,)), parts)
    sent = [rotate(sent[m - 1], "zh", m) for m in (1, 2, 3)]
    return last([kept] + sent)


def solution(mesh):
    axes = ("zh", "zz", "x", "vrow", "vcol")
    fine = Mesh(mesh.devices.reshape(-1, 2, NX, 2, 4), axes)
    field = ("zh", "zz", "x")
    held = (
        P(("vrow", "vcol"), field, None, None),
        P(("vrow", "vcol"), field, None),
        P(("vrow", "vcol"), field),
    )
    return jax.shard_map(
        on_device,
        mesh=fine,
        in_specs=held,
        out_specs=P(("vrow", *field), None, None, "vcol", None, None),
        check_vma=False,
    )
```

```python
import functools

import jax
import jax.numpy as jnp
from jax import lax
from jax.experimental import pallas as pl
from jax.experimental.pallas import tpu as pltpu
from jax.sharding import Mesh, PartitionSpec as P


SBLK = 12
OCC = 6
BLOCK = 256
VS = 128
CUT = 5 * VS
ROWS = (CUT, 2 * OCC * VS - CUT)
PARTS = [pl.ds(v, 16) for v in range(0, VS, 16)]
NX = 4
NSAMP = 98304

STEPS = 2730.0
TOP = 32767.0
BIAS = 32768.0


VM = pl.BlockSpec(memory_space=pltpu.VMEM)


def on_chip(f, out_shape, arrays, scratch, flops, aliases={}):
    arrays = [pltpu.with_memory_space_constraint(a, pltpu.VMEM) for a in arrays]
    many = isinstance(out_shape, tuple)
    return pl.pallas_call(
        f,
        out_shape=out_shape,
        in_specs=[VM] * len(arrays),
        out_specs=(VM,) * len(out_shape) if many else VM,
        scratch_shapes=scratch,
        input_output_aliases=aliases,
        cost_estimate=pl.CostEstimate(flops=flops, transcendentals=0, bytes_accessed=0),
        compiler_params=pltpu.CompilerParams(vmem_limit_bytes=12 << 20),
    )(*arrays)


def rotate(array, axis, shift):
    n = lax.axis_size(axis)
    return lax.ppermute(array, axis, [(i, i ^ shift) for i in range(n)])


def exponent(largest):
    return jnp.clip(jnp.ceil(jnp.log2(largest)), -100.0, 100.0)


def coded(values, exp):
    q = jnp.round((exp - jnp.log2(values)) * STEPS) - BIAS
    q = jnp.clip(q, -BIAS, TOP)
    return q.astype(jnp.int32).astype(jnp.int16)


def decoded(codes, exp):
    q = codes.astype(jnp.int32).astype(jnp.float32)
    return jnp.where(q >= TOP, 0.0, jnp.exp2((exp - BIAS / STEPS) - q * (1.0 / STEPS)))


def relay_kernel(blocks, a, b, held, sems):
    copies = [
        pltpu.make_async_copy(blocks.at[part], held.at[part], sems.at[i])
        for i, part in enumerate(PARTS)
    ]
    for copy in copies:
        copy.start()
    for part, copy in zip(PARTS, copies):
        copy.wait()
        for o in range(OCC):
            both = jnp.swapaxes(held[part, o], 0, 1)
            for c in range(2):
                to = (2 * o + c) * VS + part.start
                half, to = (a, to) if to < CUT else (b, to - CUT)
                half[to : to + part.size, :] = both[c]


def relaid(blocks):
    return pl.pallas_call(
        relay_kernel,
        out_shape=tuple(pltpu.VMEM((rows, BLOCK), jnp.bfloat16) for rows in ROWS),
        in_specs=[pl.BlockSpec(memory_space=pltpu.HBM)],
        out_specs=(VM,) * 2,
        scratch_shapes=[
            pltpu.VMEM(blocks.shape, jnp.bfloat16),
            pltpu.SemaphoreType.DMA((len(PARTS),)),
        ],
        compiler_params=pltpu.CompilerParams(vmem_limit_bytes=12 << 20),
    )(pltpu.with_memory_space_constraint(blocks, pltpu.HBM))


def tag_kernel(ids, count, a, b, tagged_a, tagged_b, tags):
    lane = lax.broadcasted_iota(jnp.int32, (16, BLOCK), 1)
    word = jnp.full((16, BLOCK), SBLK, jnp.int32)
    for o in range(OCC):
        word = jnp.where((lane == o) & (o < count[0]), ids[o], word)
    word = word.astype(jnp.float32).astype(jnp.bfloat16)
    tags[...] = word
    for half, out, rows in ((a, tagged_a, ROWS[0]), (b, tagged_b, ROWS[1])):
        out[:rows] = half[...]
        out[rows:] = word


def tagged(ids, count, halves):
    more = (pltpu.VMEM((rows + 16, BLOCK), jnp.bfloat16) for rows in ROWS)
    smem = pl.BlockSpec(memory_space=pltpu.SMEM)
    return pl.pallas_call(
        tag_kernel,
        out_shape=(*more, pltpu.VMEM((16, BLOCK), jnp.bfloat16)),
        in_specs=[smem, smem, VM, VM],
        out_specs=(VM,) * 3,
        cost_estimate=pl.CostEstimate(flops=2 * 256**3, transcendentals=0, bytes_accessed=0),
        compiler_params=pltpu.CompilerParams(vmem_limit_bytes=12 << 20),
    )(ids, count, *(pltpu.with_memory_space_constraint(h, pltpu.VMEM) for h in halves))


def ids_of(ref):
    at = ref.shape[0] - 16
    tags = ref[at : at + 16, :VS].astype(jnp.float32)[:1]
    lane = lax.broadcasted_iota(jnp.int32, (1, VS), 1)
    weight = jnp.zeros((1, VS), jnp.float32)
    for o in range(OCC):
        weight = jnp.where(lane == o, float(16**o), weight)
    word = jnp.sum(tags * weight).astype(jnp.int32)
    return [(word >> (4 * o)) & 15 for o in range(OCC)]


def slot_of_halves(a, b, o):
    parts = [
        a[r : r + VS, :] if r < CUT else b[r - CUT : r - CUT + VS, :]
        for r in (2 * o * VS, (2 * o + 1) * VS)
    ]
    return jnp.concatenate(parts, axis=0)


def table_kernel(n, gathers, *refs):
    col_tags, row_tags, refs = refs[:2], refs[2 : 2 + n], refs[2 + n :]
    if gathers:
        (a0, b0, a1, b1), refs = refs[:4], refs[4:]
        rows = (a0, b0)
    else:
        cols, rows, refs = refs[0], refs[1 : 1 + 2 * n], refs[1 + 2 * n :]
    outs, refs = refs[:NX], refs[NX:]
    if gathers:
        cols, refs = refs[0], refs[1:]
        for s, halves in enumerate(((a0, b0), (a1, b1))):
            for o in range(OCC):
                cols[s, o] = slot_of_halves(*halves, o)
    slot_of, acc = refs
    x, core = lax.axis_index("x"), lax.axis_index("vrow")
    for s, ref in enumerate(col_tags):
        ids = ids_of(ref)
        for k in range(SBLK + 1):
            slot_of[s, k] = -1
        for o in range(OCC):
            slot_of[s, ids[o]] = o
        slot_of[s, SBLK] = -1
    row_ids = [ids_of(ref) for ref in row_tags]
    for j in range(n):
        largest = None
        for s in range(2):
            total = None
            for o in range(OCC):
                slot = slot_of[s, row_ids[j][o]]
                m = slot_of_halves(*rows[2 * j : 2 * j + 2], o)
                m = jnp.where(slot >= 0, m, jnp.zeros_like(m))
                d = lax.dot_general(
                    m,
                    cols[s, jnp.maximum(slot, 0)],
                    (((1,), (1,)), ((), ())),
                    preferred_element_type=jnp.float32,
                )
                total = d if total is None else total + d
            acc[s] = total
            top = jnp.max(total)
            largest = top if largest is None else jnp.maximum(largest, top)
        exp = exponent(jnp.full((16, VS), largest, jnp.float32))
        for k in range(1, NX):
            outs[k][j, 256:272, :] = exp.astype(jnp.int32).astype(jnp.int16)
        for s in range(2):
            r = core if s == 0 else 1 - core
            for k in range(NX):
                there = lax.bitwise_xor(x, k) * 16
                for zz in range(2):
                    for a in range(2):
                        at = pl.ds(pl.multiple_of(there + a * VS + zz * 64, 16), 16)
                        for b in range(2):
                            v = acc[s, at, pl.ds(b * VS, VS)]
                            to = pl.multiple_of(r * 128 + (b * 64 + (zz * 2 + a) * 16), 16)
                            if k:
                                v = coded(v, exp)
                            outs[k][j, pl.ds(to, 16), :] = v


def tables(col_tags, row_tags, arrays, gathers=False):
    n = len(row_tags)
    kept = pltpu.VMEM((n, 256, VS), jnp.float32)
    sent = pltpu.VMEM((n, 272, VS), jnp.int16)
    outs = (kept,) + (sent,) * (NX - 1)
    if gathers:
        outs += (pltpu.VMEM((2, OCC, 2 * VS, BLOCK), jnp.bfloat16),)
    return on_chip(
        functools.partial(table_kernel, n, gathers),
        outs,
        [*col_tags, *row_tags, *arrays],
        [pltpu.SMEM((2, 16), jnp.int32), pltpu.VMEM((2, 256, 256), jnp.float32)],
        n * 12 * 2 * 256**3,
    )


def sum_kernel(n, *refs):
    mine, (kept, sent) = refs[:NX], refs[NX:]
    zz = lax.axis_index("zz")
    for j in range(n):
        exps = [
            mine[k][j, 256:272, :].astype(jnp.int32).astype(jnp.float32)[:1] for k in range(1, NX)
        ]
        for half, out in ((zz, kept), (1 - zz, sent)):
            for rb in range(4):
                part = pl.ds(pl.multiple_of(rb * 64 + half * 32, 32), 32)
                total = mine[0][j, part, :]
                for k in range(1, NX):
                    total = total + decoded(mine[k][j, part, :], exps[k - 1])
                out[j, rb * 32 : rb * 32 + 32, :] = total


def summed(pieces):
    n = pieces[0].shape[0]
    return on_chip(
        functools.partial(sum_kernel, n),
        (pltpu.VMEM((n, 128, VS), jnp.float32),) * 2,
        pieces,
        [],
        n * 4 * 2 * 256**3,
    )


def pair_kernel(shifts, *refs):
    g = len(shifts)
    ins, outs, (acc, exps) = refs[: 2 * g], refs[2 * g : 2 * g + 4], refs[2 * g + 4 :]
    y, zh = lax.axis_index("vcol"), lax.axis_index("zh")
    for i, group in enumerate(shifts):
        for j, shift in enumerate(group):
            p = lax.bitwise_xor(y, shift)
            total = ins[2 * i][j] + ins[2 * i + 1][j]
            acc[p] = total
            exps[p] = exponent(jnp.full((16, VS), jnp.max(total), jnp.float32))
    outs[0][...] = acc[zh]
    for m in range(1, 4):
        p = lax.bitwise_xor(zh, m)
        exp = exps[p]
        outs[m][128:144, :] = exp.astype(jnp.int32).astype(jnp.int16)
        for part in range(4):
            rows = pl.ds(part * 32, 32)
            outs[m][rows, :] = coded(acc[p, rows, :], exp[:1])


def paired(shifts, pieces):
    return on_chip(
        functools.partial(pair_kernel, shifts),
        (pltpu.VMEM((128, VS), jnp.float32),) + (pltpu.VMEM((144, VS), jnp.int16),) * 3,
        pieces,
        [pltpu.VMEM((4, 128, VS), jnp.float32), pltpu.VMEM((4, 16, VS), jnp.float32)],
        6 * 2 * 256**3,
    )


def last_kernel(*refs):
    parts, out = refs[:4], refs[4]
    exps = [parts[m][128:144, :].astype(jnp.int32).astype(jnp.float32)[:1] for m in range(1, 4)]
    for r in range(2):
        for b in range(2):
            rows = pl.ds((r * 2 + b) * 32, 32)
            total = parts[0][rows, :]
            for m in range(1, 4):
                total = total + decoded(parts[m][rows, :], exps[m - 1])
            total = total / NSAMP
            for a in range(2):
                out[:, a, r, 0, b, :] = total[a * 16 : (a + 1) * 16]


def last(parts):
    return on_chip(
        last_kernel,
        jax.ShapeDtypeStruct((16, 2, 2, 1, 2, VS), jnp.float32),
        parts,
        [],
        2 * 256**3,
    )


def on_device(blocks, block_ids, block_counts):
    a, b = relaid(blocks)
    tagged_a, tagged_b, tags = tagged(block_ids.reshape(OCC), block_counts.reshape(1), (a, b))
    up = [rotate(a, "vcol", 1), rotate(tagged_b, "vcol", 1)]
    down = [rotate(tagged_a, "vcol", 3), rotate(b, "vcol", 3)]
    sib = [rotate(a, "vrow", 1), rotate(tagged_b, "vrow", 1)]
    far_tags = rotate(tags, "vcol", 2)
    second = [rotate(up[0], "vcol", 3), rotate(down[1], "vcol", 1)]
    col_tags = [tags, sib[1]]

    def exchanged(pieces):
        return [pieces[0]] + [rotate(pieces[k], "x", k) for k in (1, 2, 3)]

    *here, cols = tables(col_tags, [tags], [a, b, *sib], gathers=True)
    near = tables(col_tags, [up[1], down[0]], [cols, *up, *down])
    far = tables(col_tags, [far_tags], [cols, *second])
    parts = []
    for pieces in (here, near, far):
        pieces = exchanged(pieces)
        kept, sent = summed(pieces)
        parts += [kept, rotate(sent, "zz", 1)]
    kept, *sent = paired(((0,), (1, 3), (2,)), parts)
    sent = [rotate(sent[m - 1], "zh", m) for m in (1, 2, 3)]
    return last([kept] + sent)


def solution(mesh):
    axes = ("zh", "zz", "x", "vrow", "vcol")
    fine = Mesh(mesh.devices.reshape(-1, 2, NX, 2, 4), axes)
    field = ("zh", "zz", "x")
    held = (
        P(("vrow", "vcol"), field, None, None),
        P(("vrow", "vcol"), field, None),
        P(("vrow", "vcol"), field),
    )
    return jax.shard_map(
        on_device,
        mesh=fine,
        in_specs=held,
        out_specs=P(("vrow", *field), None, None, "vcol", None, None),
        check_vma=False,
    )
```
